32 devices in a mesh: frames: 2 (over x), date: 8 (over z, y), row: 2 (over core).
Axes of the slice: x: 2, y: 2, z: 4, core: 2. Of those that a mesh axis runs over, the one named last changes fastest.
Arguments:
- intensity: float32 [128, 512, 512], P(('frames', 'date'), 'row'), parts along dimension 0, may hold values from 0.05 to 20
Outputs:
- filtered: float32 [128, 512, 512], P(('frames', 'date'), 'row'), parts along dimension 0
- change: float32 [128, 512, 512], P(('frames', 'date'), 'row'), parts along dimension 0
The draws below stay inside these ranges and needn't reach their ends.
There are 2 independent parts, one for each index of `frames`. The reference program is written for one: setup_inputs(seed, part) draws one part's arguments, and reference() takes and returns one part's arrays. A program takes and returns all parts, laid end to end along the dimension named above; each array names one. Nothing has to cross between parts.
All inputs are finite; a program needn't handle non-finite values.
Results may differ from the reference program's by a relative error of at most 0.00002.
Values sent between devices are 32-bit elements; how exact they have to be, the bound alone decides.
No kernel may reach another device: no remote copies, remote signals or barrier semaphores. Data moves between devices by JAX's collectives and lax.ppermute only.
A program may use at most 64 MiB of HBM per device.

```python
import math
import jax
import jax.numpy as jnp

RADIUS = 3
COLS = 512
DATES = 64
ROWS = 512


def steps_of(rng, shape, split, least, high):
    level = 1.0
    for position, shards_of in split:
        draws = jax.random.uniform(jax.random.fold_in(jax.random.fold_in(rng, 6), position), (shards_of,), jnp.float32, least / len(split), high / len(split))
        level = level * jnp.repeat(jnp.exp(draws), shape[position] // shards_of).reshape((-1,) + (1,) * (len(shape) - 1 - position))
    return level


def setup_inputs(seed: int = 0, part: int = 0) -> dict:
    keys = jax.random.split(jax.random.key(seed), 2)
    part_keys = jax.random.split(jax.random.fold_in(keys[1], part), 2)
    intensity = jnp.clip(jnp.exp(math.log(20.0) - 5.9914645 * jax.random.uniform(part_keys[0], (DATES, ROWS, COLS), jnp.float32) ** steps_of(part_keys[0], (DATES, ROWS, COLS), ((0, 8), (1, 2)), -0.2, 0.2)), 0.05, 20.0)
    return dict(intensity=intensity)


def window_sum(field):
    width = 2 * RADIUS + 1
    padded = jnp.pad(field, ((0, 0), (RADIUS, RADIUS), (RADIUS, RADIUS)))
    rows_n = field.shape[1]
    cols_n = field.shape[2]
    across = padded[:, 0:rows_n, :]
    for offset in range(1, width):
        across = across + padded[:, offset:offset + rows_n, :]
    total = across[:, :, 0:cols_n]
    for offset in range(1, width):
        total = total + across[:, :, offset:offset + cols_n]
    return total


def reference(intensity):
    ones = jnp.ones((1, intensity.shape[1], intensity.shape[2]), jnp.float32)
    count = window_sum(ones)
    local_mean = window_sum(intensity) / count
    ratio_sum = jnp.sum(intensity / local_mean, axis=0)
    filtered = local_mean * ratio_sum[None] / jnp.float32(DATES)
    logged = jnp.log(filtered)
    change = jnp.concatenate([logged[1:] - logged[:-1], jnp.zeros_like(logged[:1])], axis=0)
    return filtered, change
```

```python
import functools

import jax
import jax.numpy as jnp
from jax import lax
from jax.experimental import pallas as pl
from jax.experimental.pallas import tpu as pltpu
from jax.sharding import PartitionSpec as P

RADIUS = 3
LANES = 128
SUBLANES = 8
MIB = 1 << 20


def count_1d(places, extent):
    below = jnp.minimum(places, RADIUS)
    above = jnp.minimum(extent - 1 - places, RADIUS)
    return (below + above + 1).astype(jnp.float32)


def cell_count(row, col, rows_total, cols_total):
    shape = (SUBLANES, LANES)
    rows = row + lax.broadcasted_iota(jnp.int32, shape, 0)
    cols = col + lax.broadcasted_iota(jnp.int32, shape, 1)
    return count_1d(rows, rows_total) * count_1d(cols, cols_total)


def lane_shift(tiles, distance):
    lane = lax.broadcasted_iota(jnp.int32, tiles[0].shape, 1)
    zero = jnp.zeros_like(tiles[0])
    turned = [pltpu.roll(tile, (-distance) % LANES, 1) for tile in tiles]
    if distance > 0:
        beside = turned[1:] + [zero]
        own = lane < LANES - distance
    else:
        beside = [zero] + turned[:-1]
        own = lane >= -distance
    return [jnp.where(own, a, b) for a, b in zip(turned, beside)]


def window_tiles(load, tiles_n):
    across = []
    for j in range(tiles_n):
        x = [load(j, k) for k in range(-RADIUS, RADIUS + 1)]
        across.append(((x[0] + x[1]) + (x[2] + x[3])) + ((x[4] + x[5]) + x[6]))
    after = lane_shift(across, 1)
    left = [a + b for a, b in zip(lane_shift(across, -1), across)]
    right = [a + b for a, b in zip(across, after)]
    far_left = lane_shift(left, -2)
    far_right = lane_shift(right, 2)
    return [(far_left[j] + left[j]) + (after[j] + far_right[j]) for j in range(tiles_n)]


def window_kernel(parts_n, rows_total, place, image, above, below, sums, first, *rest):
    parts, (held, sem) = rest[:parts_n], rest[parts_n:]
    dates_n, rows_n, cols_n = image.shape
    tiles_n = cols_n // LANES
    part_rows = rows_n // parts_n
    me, row_first, has_above, has_below = place[0], place[1], place[2], place[3]
    copies = []
    for j in range(tiles_n):
        lanes = pl.ds(j * LANES, LANES)
        copy = pltpu.make_async_copy(
            image.at[:, :, lanes], held.at[:, j, pl.ds(SUBLANES, rows_n), :], sem.at[j]
        )
        copy.start()
        copies.append(copy)
    keep_above = (has_above > 0).astype(jnp.float32)
    keep_below = (has_below > 0).astype(jnp.float32)
    for t in range(dates_n):
        for j in range(tiles_n):
            lanes = pl.ds(j * LANES, LANES)
            held[t, j, SUBLANES - RADIUS : SUBLANES, :] = above[t, :, lanes] * keep_above
            held[t, j, SUBLANES + rows_n : SUBLANES + rows_n + RADIUS, :] = below[t, :, lanes] * keep_below
    for copy in copies:
        copy.wait()
    for k in range(parts_n):
        base = (me ^ k) * part_rows

        @pl.loop(0, part_rows // SUBLANES)
        def _(step):
            inside = pl.multiple_of(step * SUBLANES, SUBLANES)
            row = pl.multiple_of(base + inside, SUBLANES)
            ratio = [jnp.zeros((SUBLANES, LANES), jnp.float32)] * tiles_n
            for t in range(dates_n):
                total = window_tiles(
                    lambda j, d: held[t, j, pl.ds(row + SUBLANES + d, SUBLANES), :], tiles_n
                )
                for j in range(tiles_n):
                    sums[t, j, pl.ds(row, SUBLANES), :] = total[j]
                    if t == 0:
                        first[j, pl.ds(row, SUBLANES), :] = total[j]
                    ratio[j] = ratio[j] + held[t, j, pl.ds(row + SUBLANES, SUBLANES), :] / total[j]
            for j in range(tiles_n):
                count = cell_count(row_first + row, j * LANES, rows_total, cols_n)
                parts[k][pl.ds(inside, SUBLANES), pl.ds(j * LANES, LANES)] = ratio[j] * count


def window_call(image, above, below, place, parts_n, rows_total):
    dates_n, rows_n, cols_n = image.shape
    tiles_n = cols_n // LANES
    f32 = jnp.float32
    vmem = pl.BlockSpec(memory_space=pltpu.VMEM)
    out = pl.pallas_call(
        functools.partial(window_kernel, parts_n, rows_total),
        out_shape=[
            jax.ShapeDtypeStruct((dates_n, tiles_n, rows_n, LANES), f32),
            jax.ShapeDtypeStruct((tiles_n, rows_n, LANES), f32),
        ]
        + [jax.ShapeDtypeStruct((rows_n // parts_n, cols_n), f32)] * parts_n,
        in_specs=[
            pl.BlockSpec(memory_space=pltpu.SMEM),
            pl.BlockSpec(memory_space=pltpu.HBM),
            vmem,
            vmem,
        ],
        out_specs=[vmem] * (2 + parts_n),
        scratch_shapes=[
            pltpu.VMEM((dates_n, tiles_n, rows_n + 2 * SUBLANES, LANES), f32),
            pltpu.SemaphoreType.DMA((tiles_n,)),
        ],
        compiler_params=pltpu.CompilerParams(vmem_limit_bytes=24 * MIB),
        cost_estimate=pl.CostEstimate(flops=30 * image.size, bytes_accessed=8 * image.size, transcendentals=0),
        name="window",
    )(place, pltpu.with_memory_space_constraint(image, pltpu.HBM), above, below)
    return out[0], out[1], out[2:]


def change_kernel(dates_n, place, sums, after, change, ahead):
    step = pl.program_id(0)
    tiles_n = sums.shape[1]

    for j in range(tiles_n):
        lanes = pl.ds(j * LANES, LANES)
        logs = [jnp.log(sums[t, j]) for t in range(dates_n)]
        for t in range(dates_n - 1):
            change[t, :, lanes] = logs[t + 1] - logs[t]
        last = jnp.log(after[j]) - logs[dates_n - 1]
        change[dates_n - 1, :, lanes] = jnp.where(place[0] > 0, jnp.zeros_like(last), last)


def change_call(sums, after, is_last, block):
    dates_n, tiles_n, rows_n, _ = sums.shape
    cols_n = tiles_n * LANES
    return pl.pallas_call(
        functools.partial(change_kernel, dates_n),
        grid=(rows_n // block,),
        out_shape=jax.ShapeDtypeStruct((dates_n, rows_n, cols_n), jnp.float32),
        in_specs=[
            pl.BlockSpec(memory_space=pltpu.SMEM),
            pl.BlockSpec((dates_n, tiles_n, block, LANES), lambda i: (0, 0, i, 0)),
            pl.BlockSpec((tiles_n, block, LANES), lambda i: (0, i, 0)),
        ],
        out_specs=pl.BlockSpec((dates_n, block, cols_n), lambda i: (0, i, 0)),
        scratch_shapes=[pltpu.VMEM((SUBLANES, LANES), jnp.float32)],
        compiler_params=pltpu.CompilerParams(vmem_limit_bytes=16 * MIB),
        cost_estimate=pl.CostEstimate(flops=10 * sums.size, bytes_accessed=8 * sums.size, transcendentals=sums.size),
        name="change",
    )(is_last, sums, after)


def scale_kernel(parts_n, rows_total, dates_total, place, sums, *rest):
    totals, filtered = rest[:parts_n], rest[parts_n]
    dates_n, tiles_n, block, _ = sums.shape
    cols_n = tiles_n * LANES
    step = pl.program_id(0)
    for k in range(parts_n):

        @pl.when(step == k)
        def _():
            base = place[1] + (place[0] ^ k) * block

            @pl.loop(0, block // SUBLANES)
            def _(i):
                row = pl.multiple_of(i * SUBLANES, SUBLANES)
                for j in range(tiles_n):
                    lanes = pl.ds(j * LANES, LANES)
                    count = cell_count(base + row, j * LANES, rows_total, cols_n)
                    scale = totals[k][pl.ds(row, SUBLANES), lanes] / (count * dates_total)
                    for t in range(dates_n):
                        filtered[t, pl.ds(row, SUBLANES), lanes] = sums[t, j, pl.ds(row, SUBLANES), :] * scale


def scale_call(sums, totals, place, rows_total, dates_total):
    dates_n, tiles_n, rows_n, _ = sums.shape
    cols_n = tiles_n * LANES
    parts_n = len(totals)
    block = rows_n // parts_n
    return pl.pallas_call(
        functools.partial(scale_kernel, parts_n, rows_total, float(dates_total)),
        grid_spec=pltpu.PrefetchScalarGridSpec(
            num_scalar_prefetch=1,
            grid=(parts_n,),
            in_specs=[pl.BlockSpec((dates_n, tiles_n, block, LANES), lambda i, place: (0, 0, i ^ place[0], 0))]
            + [pl.BlockSpec(memory_space=pltpu.VMEM)] * parts_n,
            out_specs=pl.BlockSpec((dates_n, block, cols_n), lambda i, place: (0, i ^ place[0], 0)),
        ),
        out_shape=jax.ShapeDtypeStruct((dates_n, rows_n, cols_n), jnp.float32),
        compiler_params=pltpu.CompilerParams(vmem_limit_bytes=16 * MIB),
        cost_estimate=pl.CostEstimate(flops=2 * sums.size, bytes_accessed=8 * sums.size, transcendentals=0),
        name="scale",
    )(place, sums, *totals)


def crossed(block, axis, bits):
    return lax.ppermute(block, axis, [(i, i ^ bits) for i in range(lax.axis_size(axis))])


def halo_rows(image, axis):
    count = lax.axis_size(axis)
    index = lax.axis_index(axis)
    head = image[:, :RADIUS]
    tail = image[:, image.shape[1] - RADIUS :]
    if count == 2:
        other = lax.ppermute(jnp.where(index == 0, tail, head), axis, [(0, 1), (1, 0)])
        return other, other
    above = lax.ppermute(tail, axis, [(i, i + 1) for i in range(count - 1)])
    below = lax.ppermute(head, axis, [(i + 1, i) for i in range(count - 1)])
    return above, below


def parts_of(group, rows_n):
    if group & (group - 1):
        return 1
    parts = min(4, group)
    return parts if rows_n % (parts * SUBLANES) == 0 else 1


def on_device(image):
    dates_n, rows_n, cols_n = image.shape
    row_groups, date_groups = lax.axis_size("row"), lax.axis_size("date")
    row_index, date_index = lax.axis_index("row"), lax.axis_index("date")
    rows_total = rows_n * row_groups
    dates_total = dates_n * date_groups
    parts_n = parts_of(date_groups, rows_n)

    above, below = halo_rows(image, "row")
    place = jnp.stack(
        [
            date_index % parts_n,
            row_index * rows_n,
            (row_index > 0).astype(jnp.int32),
            (row_index < row_groups - 1).astype(jnp.int32),
        ]
    ).astype(jnp.int32)
    sums, first, parts = window_call(image, above, below, place, parts_n, rows_total)

    if parts_n == 1:
        totals = [lax.psum(parts[0], "date")]
    else:
        total = parts[0]
        for k in range(1, parts_n):
            total = total + crossed(parts[k], "date", k)
        bits = parts_n
        while bits < date_groups:
            total = total + crossed(total, "date", bits)
            bits *= 2
        totals = [total] + [crossed(total, "date", k) for k in range(1, parts_n)]

    after = lax.ppermute(first, "date", [(i + 1, i) for i in range(date_groups - 1)])
    is_last = (date_index == date_groups - 1).astype(jnp.int32).reshape(1)
    change = change_call(sums, after, is_last, min(rows_n, 32))
    filtered = scale_call(sums, totals, place, rows_total, dates_total)
    return filtered, change


def solution(mesh):
    spec = P(("frames", "date"), "row", None)
    return jax.shard_map(on_device, mesh=mesh, in_specs=(spec,), out_specs=(spec, spec), check_vma=False)
```

```python
import functools

import jax
import jax.numpy as jnp
from jax import lax
from jax.experimental import pallas as pl
from jax.experimental.pallas import tpu as pltpu
from jax.sharding import PartitionSpec as P


RADIUS = 3
LANES = 128
SUBLANES = 8
MIB = 1 << 20


def count_1d(places, extent):
    below = jnp.minimum(places, RADIUS)
    above = jnp.minimum(extent - 1 - places, RADIUS)
    return (below + above + 1).astype(jnp.float32)


def cell_count(row, col, rows_total, cols_total):
    shape = (SUBLANES, LANES)
    rows = row + lax.broadcasted_iota(jnp.int32, shape, 0)
    cols = col + lax.broadcasted_iota(jnp.int32, shape, 1)
    return count_1d(rows, rows_total) * count_1d(cols, cols_total)


def lane_shift(tiles, distance):
    lane = lax.broadcasted_iota(jnp.int32, tiles[0].shape, 1)
    zero = jnp.zeros_like(tiles[0])
    turned = [pltpu.roll(tile, (-distance) % LANES, 1) for tile in tiles]
    if distance > 0:
        beside = turned[1:] + [zero]
        own = lane < LANES - distance
    else:
        beside = [zero] + turned[:-1]
        own = lane >= -distance
    return [jnp.where(own, a, b) for a, b in zip(turned, beside)]


def window_tiles(load, tiles_n):
    across = []
    for j in range(tiles_n):
        x = [load(j, k) for k in range(-RADIUS, RADIUS + 1)]
        across.append(((x[0] + x[1]) + (x[2] + x[3])) + ((x[4] + x[5]) + x[6]))
    after = lane_shift(across, 1)
    left = [a + b for a, b in zip(lane_shift(across, -1), across)]
    right = [a + b for a, b in zip(across, after)]
    far_left = lane_shift(left, -2)
    far_right = lane_shift(right, 2)
    return [(far_left[j] + left[j]) + (after[j] + far_right[j]) for j in range(tiles_n)]


def window_kernel(parts_n, rows_total, place, image, above, below, sums, *rest):
    parts, (held, ratios, sem) = rest[:parts_n], rest[parts_n:]
    dates_n, rows_n, cols_n = image.shape
    tiles_n = cols_n // LANES
    part_rows = rows_n // parts_n
    me, row_first = place[0], place[1]

    def copies(c):
        return [
            pltpu.make_async_copy(
                image.at[:, pl.ds(c * part_rows, part_rows), pl.ds(j * LANES, LANES)],
                held.at[:, j, pl.ds(SUBLANES + c * part_rows, part_rows), :],
                sem.at[c, j],
            )
            for j in range(tiles_n)
        ]

    for c in range(parts_n):
        for copy in copies(c):
            copy.start()
    fill_rims(place, held, above, below)
    for copy in copies(0):
        copy.wait()
    for c in range(parts_n):
        if c + 1 < parts_n:
            for copy in copies(c + 1):
                copy.wait()

        @pl.loop(0, part_rows // SUBLANES)
        def _(step):
            inside = pl.multiple_of(step * SUBLANES, SUBLANES)
            row = pl.multiple_of(c * part_rows + inside, SUBLANES)
            ratio = [jnp.zeros((SUBLANES, LANES), jnp.float32)] * tiles_n
            for t in range(dates_n):
                total = window_tiles(
                    lambda j, d: held[t, j, pl.ds(row + SUBLANES + d, SUBLANES), :], tiles_n
                )
                for j in range(tiles_n):
                    sums[t, j, pl.ds(row, SUBLANES), :] = total[j]
                    ratio[j] = ratio[j] + held[t, j, pl.ds(row + SUBLANES, SUBLANES), :] / total[j]
            for j in range(tiles_n):
                count = cell_count(row_first + row, j * LANES, rows_total, cols_n)
                ratios[pl.ds(inside, SUBLANES), pl.ds(j * LANES, LANES)] = ratio[j] * count

        for k in range(parts_n):

            @pl.when((me ^ k) == c)
            def _():
                parts[k][...] = ratios[...]


def fill_rims(place, held, above, below):
    dates_n, tiles_n, padded_n, _ = held.shape
    end = padded_n - SUBLANES
    keep_above = (place[2] > 0).astype(jnp.float32)
    keep_below = (place[3] > 0).astype(jnp.float32)
    for t in range(dates_n):
        for j in range(tiles_n):
            lanes = pl.ds(j * LANES, LANES)
            held[t, j, SUBLANES - RADIUS : SUBLANES, :] = above[t, :, lanes] * keep_above
            held[t, j, end : end + RADIUS, :] = below[t, :, lanes] * keep_below


def window_call(image, above, below, place, parts_n, rows_total):
    dates_n, rows_n, cols_n = image.shape
    tiles_n = cols_n // LANES
    f32 = jnp.float32
    vmem = pl.BlockSpec(memory_space=pltpu.VMEM)
    part = (rows_n // parts_n, cols_n)
    out = pl.pallas_call(
        functools.partial(window_kernel, parts_n, rows_total),
        out_shape=[jax.ShapeDtypeStruct((dates_n, tiles_n, rows_n, LANES), f32)]
        + [jax.ShapeDtypeStruct(part, f32)] * parts_n,
        in_specs=[
            pl.BlockSpec(memory_space=pltpu.SMEM),
            pl.BlockSpec(memory_space=pltpu.HBM),
            vmem,
            vmem,
        ],
        out_specs=[vmem] * (1 + parts_n),
        scratch_shapes=[
            pltpu.VMEM((dates_n, tiles_n, rows_n + 2 * SUBLANES, LANES), f32),
            pltpu.VMEM(part, f32),
            pltpu.SemaphoreType.DMA((parts_n, tiles_n)),
        ],
        compiler_params=pltpu.CompilerParams(vmem_limit_bytes=16 * MIB),
        cost_estimate=pl.CostEstimate(flops=30 * image.size, bytes_accessed=8 * image.size, transcendentals=0),
        name="window",
    )(place, pltpu.with_memory_space_constraint(image, pltpu.HBM), above, below)
    return out[0], out[1:]


def change_kernel(sums, change, held, sem):
    dates_n, tiles_n, rows_n, _ = sums.shape
    block = held.shape[2]
    copies = []
    for c in range(rows_n // block):

        @pl.loop(0, block // SUBLANES)
        def _(step):
            inside = pl.multiple_of(step * SUBLANES, SUBLANES)
            row = pl.multiple_of(c * block + inside, SUBLANES)
            for j in range(tiles_n):
                before = jnp.log(sums[0, j, pl.ds(row, SUBLANES), :])
                for t in range(dates_n - 1):
                    ahead = jnp.log(sums[t + 1, j, pl.ds(row, SUBLANES), :])
                    held[c, t, pl.ds(inside, SUBLANES), pl.ds(j * LANES, LANES)] = ahead - before
                    before = ahead

        copy = pltpu.make_async_copy(
            held.at[c], change.at[pl.ds(0, dates_n - 1), pl.ds(c * block, block), :], sem.at[c]
        )
        copy.start()
        copies.append(copy)
    for copy in copies:
        copy.wait()


def change_call(sums, block):
    dates_n, tiles_n, rows_n, _ = sums.shape
    cols_n = tiles_n * LANES
    chunks = rows_n // block
    return pl.pallas_call(
        change_kernel,
        out_shape=jax.ShapeDtypeStruct((dates_n, rows_n, cols_n), jnp.float32),
        in_specs=[pl.BlockSpec(memory_space=pltpu.VMEM)],
        out_specs=pl.BlockSpec(memory_space=pltpu.HBM),
        scratch_shapes=[
            pltpu.VMEM((chunks, dates_n - 1, block, cols_n), jnp.float32),
            pltpu.SemaphoreType.DMA((chunks,)),
        ],
        compiler_params=pltpu.CompilerParams(vmem_limit_bytes=12 * MIB),
        cost_estimate=pl.CostEstimate(flops=2000 * sums.size, bytes_accessed=8 * sums.size, transcendentals=sums.size),
        name="change",
    )(sums)


def last_kernel(unroll, place, sums, image, above, below, _, change, held, made, sem):
    dates_n, tiles_n, rows_n, _ = sums.shape
    for j in range(tiles_n):
        held[0, j, SUBLANES : SUBLANES + rows_n, :] = image[0, :, pl.ds(j * LANES, LANES)]
    fill_rims(place, held, above, below)
    keep = place[4] == 0

    @pl.loop(0, rows_n // (SUBLANES * unroll))
    def _(step):
        for u in range(unroll):
            row = pl.multiple_of((step * unroll + u) * SUBLANES, SUBLANES)
            total = window_tiles(
                lambda j, d: held[0, j, pl.ds(row + SUBLANES + d, SUBLANES), :], tiles_n
            )
            for j in range(tiles_n):
                own = sums[dates_n - 1, j, pl.ds(row, SUBLANES), :]
                ahead = jnp.where(keep, total[j], own)
                made[pl.ds(row, SUBLANES), pl.ds(j * LANES, LANES)] = jnp.log(ahead) - jnp.log(own)

    copy = pltpu.make_async_copy(made, change.at[dates_n - 1], sem)
    copy.start()
    copy.wait()


def last_call(sums, image, above, below, place, change):
    _, tiles_n, rows_n, _ = sums.shape
    cols_n = tiles_n * LANES
    whole = pl.BlockSpec(memory_space=pltpu.VMEM)
    hbm = pl.BlockSpec(memory_space=pltpu.HBM)
    unroll = 8 if rows_n % (8 * SUBLANES) == 0 else 1
    return pl.pallas_call(
        functools.partial(last_kernel, unroll),
        out_shape=jax.ShapeDtypeStruct(change.shape, jnp.float32),
        in_specs=[pl.BlockSpec(memory_space=pltpu.SMEM), whole, whole, whole, whole, hbm],
        out_specs=hbm,
        scratch_shapes=[
            pltpu.VMEM((1, tiles_n, rows_n + 2 * SUBLANES, LANES), jnp.float32),
            pltpu.VMEM((rows_n, cols_n), jnp.float32),
            pltpu.SemaphoreType.DMA,
        ],
        input_output_aliases={5: 0},
        compiler_params=pltpu.CompilerParams(vmem_limit_bytes=12 * MIB),
        cost_estimate=pl.CostEstimate(flops=2000 * image.size, bytes_accessed=12 * image.size, transcendentals=0),
        name="last",
    )(place, sums, image, above, below, change)


def scale_kernel(k, rows_total, dates_total, place, sums, total, *rest):
    filtered, held, scale, sem = rest[-4:]
    dates_n, tiles_n, _, _ = sums.shape
    cols_n = tiles_n * LANES
    block = total.shape[0]
    first = pl.multiple_of((place[0] ^ k) * block, SUBLANES)

    @pl.loop(0, block // SUBLANES)
    def _(i):
        row = pl.multiple_of(i * SUBLANES, SUBLANES)
        for j in range(tiles_n):
            lanes = pl.ds(j * LANES, LANES)
            count = cell_count(place[1] + first + row, j * LANES, rows_total, cols_n)
            scale[pl.ds(row, SUBLANES), lanes] = total[pl.ds(row, SUBLANES), lanes] / (count * dates_total)

    copies = []
    for t in range(dates_n):
        for j in range(tiles_n):
            lanes = pl.ds(j * LANES, LANES)
            held[t, :, lanes] = sums[t, j, pl.ds(first, block), :] * scale[:, lanes]
        copy = pltpu.make_async_copy(held.at[t], filtered.at[t, pl.ds(first, block), :], sem.at[t])
        copy.start()
        copies.append(copy)
    for copy in copies:
        copy.wait()


def scale_call(sums, total, place, k, rows_total, dates_total, filtered):
    dates_n, tiles_n, rows_n, _ = sums.shape
    cols_n = tiles_n * LANES
    block = total.shape[0]
    aliased = [] if filtered is None else [filtered]
    whole = pl.BlockSpec(memory_space=pltpu.VMEM)
    hbm = pl.BlockSpec(memory_space=pltpu.HBM)
    return pl.pallas_call(
        functools.partial(scale_kernel, k, rows_total, float(dates_total)),
        in_specs=[pl.BlockSpec(memory_space=pltpu.SMEM), whole, whole] + [hbm] * len(aliased),
        out_specs=hbm,
        out_shape=jax.ShapeDtypeStruct((dates_n, rows_n, cols_n), jnp.float32),
        scratch_shapes=[
            pltpu.VMEM((dates_n, block, cols_n), jnp.float32),
            pltpu.VMEM((block, cols_n), jnp.float32),
            pltpu.SemaphoreType.DMA((dates_n,)),
        ],
        input_output_aliases={3: 0} if aliased else {},
        compiler_params=pltpu.CompilerParams(vmem_limit_bytes=12 * MIB),
        cost_estimate=pl.CostEstimate(flops=500 * sums.size, bytes_accessed=8 * sums.size, transcendentals=0),
    )(place, sums, total, *aliased)


def crossed(block, axis, bits):
    return lax.ppermute(block, axis, [(i, i ^ bits) for i in range(lax.axis_size(axis))])


def halo_rows(image, axis):
    count = lax.axis_size(axis)
    index = lax.axis_index(axis)
    head = image[:, :RADIUS]
    tail = image[:, image.shape[1] - RADIUS :]
    if count == 2:
        other = lax.ppermute(jnp.where(index == 0, tail, head), axis, [(0, 1), (1, 0)])
        return other, other
    above = lax.ppermute(tail, axis, [(i, i + 1) for i in range(count - 1)])
    below = lax.ppermute(head, axis, [(i + 1, i) for i in range(count - 1)])
    return above, below


def parts_of(group, rows_n):
    if group & (group - 1):
        return 1
    parts = min(4, group)
    return parts if rows_n % (parts * SUBLANES) == 0 else 1


def on_device(image):
    dates_n, rows_n, _ = image.shape
    row_groups, date_groups = lax.axis_size("row"), lax.axis_size("date")
    row_index, date_index = lax.axis_index("row"), lax.axis_index("date")
    rows_total = rows_n * row_groups
    dates_total = dates_n * date_groups
    parts_n = parts_of(date_groups, rows_n)

    place = jnp.stack(
        [
            date_index & (parts_n - 1),
            row_index * rows_n,
            (row_index > 0).astype(jnp.int32),
            (row_index < row_groups - 1).astype(jnp.int32),
            (date_index == date_groups - 1).astype(jnp.int32),
        ]
    ).astype(jnp.int32)
    above, below = halo_rows(image, "row")
    after = lax.ppermute(image[:1], "date", [(i + 1, i) for i in range(date_groups - 1)])
    sums, parts = window_call(image, above, below, place, parts_n, rows_total)

    if parts_n == 1:
        totals = [lax.psum(parts[0], "date")]
    else:
        total = parts[0]
        for k in range(1, parts_n):
            total = total + crossed(parts[k], "date", k)
        bits = parts_n
        while bits < date_groups:
            total = total + crossed(total, "date", bits)
            bits *= 2
        totals = [total]
        for k in range(1, parts_n):
            totals.append(crossed(total, "date", k))

    change = change_call(sums, min(rows_n, 64))
    after_above, after_below = halo_rows(after, "row")
    change = last_call(sums, after, after_above, after_below, place, change)
    filtered = None
    for k in range(parts_n):
        filtered = scale_call(sums, totals[k], place, k, rows_total, dates_total, filtered)
    return filtered, change


def solution(mesh):
    spec = P(("frames", "date"), "row", None)
    return jax.shard_map(on_device, mesh=mesh, in_specs=(spec,), out_specs=(spec, spec), check_vma=False)
```

```python
import functools

import jax
import jax.numpy as jnp
from jax import lax
from jax.experimental import pallas as pl
from jax.experimental.pallas import tpu as pltpu
from jax.sharding import PartitionSpec as P


RADIUS = 3
LANES = 128
SUBLANES = 8
MIB = 1 << 20


def count_1d(places, extent):
    below = jnp.minimum(places, RADIUS)
    above = jnp.minimum(extent - 1 - places, RADIUS)
    return (below + above + 1).astype(jnp.float32)


def cell_count(row, col, rows_total, cols_total):
    shape = (SUBLANES, LANES)
    rows = row + lax.broadcasted_iota(jnp.int32, shape, 0)
    cols = col + lax.broadcasted_iota(jnp.int32, shape, 1)
    return count_1d(rows, rows_total) * count_1d(cols, cols_total)


def lane_shift(tiles, distance):
    lane = lax.broadcasted_iota(jnp.int32, tiles[0].shape, 1)
    zero = jnp.zeros_like(tiles[0])
    turned = [pltpu.roll(tile, (-distance) % LANES, 1) for tile in tiles]
    if distance > 0:
        beside = turned[1:] + [zero]
        own = lane < LANES - distance
    else:
        beside = [zero] + turned[:-1]
        own = lane >= -distance
    return [jnp.where(own, a, b) for a, b in zip(turned, beside)]


def window_tiles(load, tiles_n):
    across = []
    for j in range(tiles_n):
        x = [load(j, k) for k in range(-RADIUS, RADIUS + 1)]
        across.append(((x[0] + x[1]) + (x[2] + x[3])) + ((x[4] + x[5]) + x[6]))
    after = lane_shift(across, 1)
    left = [a + b for a, b in zip(lane_shift(across, -1), across)]
    right = [a + b for a, b in zip(across, after)]
    far_left = lane_shift(left, -2)
    far_right = lane_shift(right, 2)
    return [(far_left[j] + left[j]) + (after[j] + far_right[j]) for j in range(tiles_n)]


def part_row(place, k, part_rows):
    return pl.multiple_of((place[0] ^ k) * part_rows, SUBLANES)


def window_kernel(k, rows_total, dates_total, place, image, above, below, sums, part, *rest):
    held = rest[-1]
    dates_n, rows_n, cols_n = image.shape
    tiles_n, part_rows = sums.shape[1], sums.shape[2]
    first = part_row(place, k, part_rows)
    end = SUBLANES + part_rows
    tiles = [(t, j, pl.ds(j * LANES, LANES)) for t in range(dates_n) for j in range(tiles_n)]
    for t, j, lanes in tiles:
        held[t, j, SUBLANES:end, :] = image[t, pl.ds(first, part_rows), lanes]

    @pl.when(first > 0)
    def _():
        for t, j, lanes in tiles:
            held[t, j, :SUBLANES, :] = image[t, pl.ds(pl.multiple_of(first - SUBLANES, SUBLANES), SUBLANES), lanes]

    @pl.when(first == 0)
    def _():
        fill_above(place, held, above)

    @pl.when(first + part_rows < rows_n)
    def _():
        for t, j, lanes in tiles:
            held[t, j, end:, :] = image[t, pl.ds(pl.multiple_of(first + part_rows, SUBLANES), SUBLANES), lanes]

    @pl.when(first + part_rows == rows_n)
    def _():
        fill_below(place, held, below)

    @pl.loop(0, part_rows // SUBLANES)
    def _(step):
        row = pl.multiple_of(step * SUBLANES, SUBLANES)
        ratio = [jnp.zeros((SUBLANES, LANES), jnp.float32)] * tiles_n
        for t in range(dates_n):
            total = window_tiles(
                lambda j, d: held[t, j, pl.ds(row + SUBLANES + d, SUBLANES), :], tiles_n
            )
            for j in range(tiles_n):
                sums[t, j, pl.ds(row, SUBLANES), :] = total[j]
                ratio[j] = ratio[j] + held[t, j, pl.ds(row + SUBLANES, SUBLANES), :] / total[j]
        for j in range(tiles_n):
            count = cell_count(place[1] + first + row, j * LANES, rows_total, cols_n)
            part[pl.ds(row, SUBLANES), pl.ds(j * LANES, LANES)] = ratio[j] * count
            if k == 0:
                rest[0][pl.ds(row, SUBLANES), pl.ds(j * LANES, LANES)] = 1.0 / (count * dates_total)


def fill_above(place, held, above):
    keep = (place[2] > 0).astype(jnp.float32)
    for t in range(held.shape[0]):
        for j in range(held.shape[1]):
            held[t, j, SUBLANES - RADIUS : SUBLANES, :] = above[t, :, pl.ds(j * LANES, LANES)] * keep


def fill_below(place, held, below):
    end = held.shape[2] - SUBLANES
    keep = (place[3] > 0).astype(jnp.float32)
    for t in range(held.shape[0]):
        for j in range(held.shape[1]):
            held[t, j, end : end + RADIUS, :] = below[t, :, pl.ds(j * LANES, LANES)] * keep


SCALARS = pl.BlockSpec(memory_space=pltpu.SMEM)
WHOLE = pl.BlockSpec(memory_space=pltpu.VMEM)
OUTER = pl.BlockSpec(memory_space=pltpu.HBM)


def window_call(image, above, below, place, k, parts_n, rows_total, dates_total):
    dates_n, rows_n, cols_n = image.shape
    tiles_n = cols_n // LANES
    part_rows = rows_n // parts_n
    outs = 2 if k == 0 else 1
    f32 = jnp.float32
    return pl.pallas_call(
        functools.partial(window_kernel, k, rows_total, float(dates_total)),
        out_shape=[
            jax.ShapeDtypeStruct((dates_n, tiles_n, part_rows, LANES), f32),
        ]
        + [jax.ShapeDtypeStruct((part_rows, cols_n), f32)] * outs,
        in_specs=[SCALARS, WHOLE, WHOLE, WHOLE],
        out_specs=[WHOLE] * (1 + outs),
        scratch_shapes=[pltpu.VMEM((dates_n, tiles_n, part_rows + 2 * SUBLANES, LANES), f32)],
        compiler_params=pltpu.CompilerParams(vmem_limit_bytes=12 * MIB),
        cost_estimate=pl.CostEstimate(flops=500 * image.size, bytes_accessed=8 * image.size, transcendentals=0),
    )(place, image, above, below)


def change_kernel(parts_n, place, *rest):
    sums = rest[:parts_n]
    change, held, sem = rest[parts_n:]
    dates_n, tiles_n, part_rows, _ = sums[0].shape
    copies = []
    for k in range(parts_n):

        @pl.loop(0, part_rows // SUBLANES)
        def _(step):
            rows = pl.ds(pl.multiple_of(step * SUBLANES, SUBLANES), SUBLANES)
            for j in range(tiles_n):
                before = jnp.log(sums[k][0, j, rows, :])
                for t in range(dates_n - 1):
                    ahead = jnp.log(sums[k][t + 1, j, rows, :])
                    held[k, t, rows, pl.ds(j * LANES, LANES)] = ahead - before
                    before = ahead

        place_rows = pl.ds(part_row(place, k, part_rows), part_rows)
        copy = pltpu.make_async_copy(held.at[k], change.at[pl.ds(0, dates_n - 1), place_rows, :], sem.at[k])
        copy.start()
        copies.append(copy)
    for copy in copies:
        copy.wait()


def change_call(sums, place):
    parts_n = len(sums)
    dates_n, tiles_n, part_rows, _ = sums[0].shape
    cols_n = tiles_n * LANES
    size = parts_n * sums[0].size
    return pl.pallas_call(
        functools.partial(change_kernel, parts_n),
        out_shape=jax.ShapeDtypeStruct((dates_n, parts_n * part_rows, cols_n), jnp.float32),
        in_specs=[SCALARS] + [WHOLE] * parts_n,
        out_specs=OUTER,
        scratch_shapes=[
            pltpu.VMEM((parts_n, dates_n - 1, part_rows, cols_n), jnp.float32),
            pltpu.SemaphoreType.DMA((parts_n,)),
        ],
        compiler_params=pltpu.CompilerParams(vmem_limit_bytes=12 * MIB),
        cost_estimate=pl.CostEstimate(flops=2000 * size, bytes_accessed=8 * size, transcendentals=size),
        name="change",
    )(place, *sums)


def last_kernel(parts_n, unroll, place, *rest):
    sums, pieces = rest[:parts_n], rest[parts_n:-7]
    above, below, _, change, held, made, sem = rest[-7:]
    dates_n, tiles_n, part_rows, _ = sums[0].shape
    start = SUBLANES
    for piece in pieces:
        for j in range(tiles_n):
            held[0, j, start : start + piece.shape[1], :] = piece[0, :, pl.ds(j * LANES, LANES)]
        start += piece.shape[1]
    fill_above(place, held, above)
    fill_below(place, held, below)
    keep = place[4] == 0
    for k in range(parts_n):
        first = part_row(place, k, part_rows)

        @pl.loop(0, part_rows // (SUBLANES * unroll))
        def _(step):
            for u in range(unroll):
                inside = pl.multiple_of((step * unroll + u) * SUBLANES, SUBLANES)
                row = pl.multiple_of(first + inside, SUBLANES)
                total = window_tiles(
                    lambda j, d: held[0, j, pl.ds(row + SUBLANES + d, SUBLANES), :], tiles_n
                )
                for j in range(tiles_n):
                    own = sums[k][dates_n - 1, j, pl.ds(inside, SUBLANES), :]
                    ahead = jnp.where(keep, total[j], own)
                    made[pl.ds(row, SUBLANES), pl.ds(j * LANES, LANES)] = jnp.log(ahead) - jnp.log(own)

    copy = pltpu.make_async_copy(made, change.at[dates_n - 1], sem)
    copy.start()
    copy.wait()


def last_call(sums, pieces, above, below, place, change):
    parts_n = len(sums)
    _, tiles_n, part_rows, _ = sums[0].shape
    rows_n, cols_n = parts_n * part_rows, tiles_n * LANES
    inputs = parts_n + len(pieces) + 3
    unroll = 8 if part_rows % (8 * SUBLANES) == 0 else 1
    return pl.pallas_call(
        functools.partial(last_kernel, parts_n, unroll),
        out_shape=jax.ShapeDtypeStruct(change.shape, jnp.float32),
        in_specs=[SCALARS] + [WHOLE] * (inputs - 1) + [OUTER],
        out_specs=OUTER,
        scratch_shapes=[
            pltpu.VMEM((1, tiles_n, rows_n + 2 * SUBLANES, LANES), jnp.float32),
            pltpu.VMEM((rows_n, cols_n), jnp.float32),
            pltpu.SemaphoreType.DMA,
        ],
        input_output_aliases={inputs: 0},
        compiler_params=pltpu.CompilerParams(vmem_limit_bytes=12 * MIB),
        cost_estimate=pl.CostEstimate(flops=2000 * rows_n * cols_n, bytes_accessed=12 * rows_n * cols_n, transcendentals=0),
        name="last",
    )(place, *sums, *pieces, above, below, change)


def scale_kernel(ks, place, *rest):
    n = len(ks)
    sums, scales = rest[:n], rest[n : 2 * n]
    filtered, held, sem = rest[-3:]
    dates_n, tiles_n, part_rows, _ = sums[0].shape
    copies = []
    for i, k in enumerate(ks):
        rows = pl.ds(part_row(place, k, part_rows), part_rows)
        for t in range(dates_n):
            for j in range(tiles_n):
                lanes = pl.ds(j * LANES, LANES)
                held[i, t, :, lanes] = sums[i][t, j] * scales[i][:, lanes]
            copy = pltpu.make_async_copy(held.at[i, t], filtered.at[t, rows, :], sem.at[i, t])
            copy.start()
            copies.append(copy)
    for copy in copies:
        copy.wait()


def scale_call(sums, scales, place, ks, rows_n, filtered):
    n = len(ks)
    dates_n, tiles_n, part_rows, _ = sums[0].shape
    cols_n = tiles_n * LANES
    size = n * sums[0].size
    aliased = [] if filtered is None else [filtered]
    return pl.pallas_call(
        functools.partial(scale_kernel, ks),
        in_specs=[SCALARS] + [WHOLE] * (2 * n) + [OUTER] * len(aliased),
        out_specs=OUTER,
        out_shape=jax.ShapeDtypeStruct((dates_n, rows_n, cols_n), jnp.float32),
        scratch_shapes=[
            pltpu.VMEM((n, dates_n, part_rows, cols_n), jnp.float32),
            pltpu.SemaphoreType.DMA((n, dates_n)),
        ],
        input_output_aliases={2 * n + 1: 0} if aliased else {},
        compiler_params=pltpu.CompilerParams(vmem_limit_bytes=12 * MIB),
        cost_estimate=pl.CostEstimate(flops=1000 * size, bytes_accessed=8 * size, transcendentals=0),
    )(place, *sums, *scales, *aliased)


def crossed(block, axis, bits):
    return lax.ppermute(block, axis, [(i, i ^ bits) for i in range(lax.axis_size(axis))])


def halo_rows(pieces, axis, is_first):
    count = lax.axis_size(axis)
    head = pieces[0][:, :RADIUS]
    tail = pieces[-1][:, pieces[-1].shape[1] - RADIUS :]
    if count == 2:
        other = lax.ppermute(jnp.where(is_first, tail, head), axis, [(0, 1), (1, 0)])
        return other, other
    above = lax.ppermute(tail, axis, [(i, i + 1) for i in range(count - 1)])
    below = lax.ppermute(head, axis, [(i + 1, i) for i in range(count - 1)])
    return above, below


def rim_kernel(place, first, final, rim):
    is_first = place[2] == 0
    rows_n = final.shape[1]
    tail = final[:, rows_n - SUBLANES :, :]
    head = first[:, :SUBLANES, :]
    rim[...] = jnp.where(is_first, tail[:, SUBLANES - RADIUS :, :], head[:, :RADIUS, :])


def rim_call(pieces, place):
    first, final = pieces[0], pieces[-1]
    return pl.pallas_call(
        rim_kernel,
        out_shape=jax.ShapeDtypeStruct((first.shape[0], RADIUS, first.shape[2]), jnp.float32),
        in_specs=[SCALARS, WHOLE, WHOLE],
        out_specs=WHOLE,
        compiler_params=pltpu.CompilerParams(vmem_limit_bytes=4 * MIB),
        name="rim",
    )(place, first, final)


def prepare_kernel(place, image, rim, early, held, sem):
    rows_n = image.shape[1]
    is_first = place[2] == 0
    start = pl.multiple_of(jnp.where(is_first, rows_n - SUBLANES, 0), SUBLANES)
    edge = pltpu.make_async_copy(image.at[:, pl.ds(start, SUBLANES), :], held, sem.at[0])
    edge.start()
    copy = pltpu.make_async_copy(image.at[pl.ds(0, 1), pl.ds(0, early.shape[1]), :], early, sem.at[1])
    copy.start()
    edge.wait()
    rim[...] = jnp.where(is_first, held[:, SUBLANES - RADIUS :, :], held[:, :RADIUS, :])
    copy.wait()


def prepare_call(image, place, cut):
    dates_n, _, cols_n = image.shape
    return pl.pallas_call(
        prepare_kernel,
        out_shape=[
            jax.ShapeDtypeStruct((dates_n, RADIUS, cols_n), jnp.float32),
            jax.ShapeDtypeStruct((1, cut, cols_n), jnp.float32),
        ],
        in_specs=[SCALARS, OUTER],
        out_specs=[WHOLE, WHOLE],
        scratch_shapes=[pltpu.VMEM((dates_n, SUBLANES, cols_n), jnp.float32), pltpu.SemaphoreType.DMA((2,))],
        compiler_params=pltpu.CompilerParams(vmem_limit_bytes=4 * MIB),
        name="prepare",
    )(place, pltpu.with_memory_space_constraint(image, pltpu.HBM))


def parts_of(group, rows_n):
    if group & (group - 1):
        return 1
    parts = min(4, group)
    return parts if rows_n % (parts * SUBLANES) == 0 else 1


def on_device(image):
    dates_n, rows_n, _ = image.shape
    row_groups, date_groups = lax.axis_size("row"), lax.axis_size("date")
    row_index, date_index = lax.axis_index("row"), lax.axis_index("date")
    rows_total = rows_n * row_groups
    dates_total = dates_n * date_groups
    parts_n = parts_of(date_groups, rows_n)

    place = jnp.stack(
        [
            date_index & (parts_n - 1),
            row_index * rows_n,
            (row_index > 0).astype(jnp.int32),
            (row_index < row_groups - 1).astype(jnp.int32),
            (date_index == date_groups - 1).astype(jnp.int32),
        ]
    ).astype(jnp.int32)
    cut = rows_n
    route = [(i + 1, i) for i in range(date_groups - 1)]
    if row_groups == 2:
        rim, early = prepare_call(image, place, cut)
        above = below = lax.ppermute(rim, "row", [(0, 1), (1, 0)])
    else:
        early = image[:1, :cut]
        above, below = halo_rows([image], "row", place[2] == 0)
    after = [lax.ppermute(early, "date", route)]
    if cut < rows_n:
        after.append(lax.ppermute(image[:1, cut:], "date", route))
    sums, parts = [], []
    for k in range(parts_n):
        made = window_call(image, above, below, place, k, parts_n, rows_total, dates_total)
        sums.append(made[0])
        parts.append(made[1])
        if k == 0:
            norm = made[2]

    if parts_n == 1:
        total = lax.psum(parts[0], "date")
    else:
        total = parts[0]
        for k in range(1, parts_n):
            total = total + crossed(parts[k], "date", k)
        bits = parts_n
        while bits < date_groups:
            total = total + crossed(total, "date", bits)
            bits *= 2
    scales = [total * norm]
    for k in range(1, parts_n):
        scales.append(crossed(scales[0], "date", k))

    change = change_call(sums, place)
    if row_groups == 2:
        after_above = after_below = lax.ppermute(rim_call(after, place), "row", [(0, 1), (1, 0)])
    else:
        after_above, after_below = halo_rows(after, "row", place[2] == 0)
    change = last_call(sums, after, after_above, after_below, place, change)
    filtered = scale_call(sums[:1], scales[:1], place, (0,), rows_n, None)
    if parts_n > 1:
        filtered = scale_call(sums[1:], scales[1:], place, tuple(range(1, parts_n)), rows_n, filtered)
    return filtered, change


def solution(mesh):
    spec = P(("frames", "date"), "row", None)
    return jax.shard_map(on_device, mesh=mesh, in_specs=(spec,), out_specs=(spec, spec), check_vma=False)
```

```python
import functools

import jax
import jax.numpy as jnp
from jax import lax
from jax.experimental import pallas as pl
from jax.experimental.pallas import tpu as pltpu
from jax.sharding import PartitionSpec as P


RADIUS = 3
LANES = 128
SUBLANES = 8
MIB = 1 << 20


def count_1d(places, extent):
    below = jnp.minimum(places, RADIUS)
    above = jnp.minimum(extent - 1 - places, RADIUS)
    return (below + above + 1).astype(jnp.float32)


def cell_count(row, col, rows_total, cols_total):
    shape = (SUBLANES, LANES)
    rows = row + lax.broadcasted_iota(jnp.int32, shape, 0)
    cols = col + lax.broadcasted_iota(jnp.int32, shape, 1)
    return count_1d(rows, rows_total) * count_1d(cols, cols_total)


def lane_shift(tiles, distance):
    lane = lax.broadcasted_iota(jnp.int32, tiles[0].shape, 1)
    zero = jnp.zeros_like(tiles[0])
    turned = [pltpu.roll(tile, (-distance) % LANES, 1) for tile in tiles]
    if distance > 0:
        beside = turned[1:] + [zero]
        own = lane < LANES - distance
    else:
        beside = [zero] + turned[:-1]
        own = lane >= -distance
    return [jnp.where(own, a, b) for a, b in zip(turned, beside)]


def window_tiles(load, tiles_n):
    across = []
    for j in range(tiles_n):
        x = [load(j, k) for k in range(-RADIUS, RADIUS + 1)]
        across.append(((x[0] + x[1]) + (x[2] + x[3])) + ((x[4] + x[5]) + x[6]))
    after = lane_shift(across, 1)
    left = [a + b for a, b in zip(lane_shift(across, -1), across)]
    right = [a + b for a, b in zip(across, after)]
    far_left = lane_shift(left, -2)
    far_right = lane_shift(right, 2)
    return [(far_left[j] + left[j]) + (after[j] + far_right[j]) for j in range(tiles_n)]


def located(kernel, parts_n, rows_n):
    def run(*refs):
        date, row = lax.axis_index("date"), lax.axis_index("row")
        place = [
            date & (parts_n - 1),
            row * rows_n,
            (row > 0).astype(jnp.int32),
            (row < lax.axis_size("row") - 1).astype(jnp.int32),
            (date == lax.axis_size("date") - 1).astype(jnp.int32),
        ]
        return kernel(place, *refs)

    return run


def part_row(place, k, part_rows):
    return pl.multiple_of((place[0] ^ k) * part_rows, SUBLANES)


def window_kernel(k, rows_total, dates_total, place, image, above, below, sums, part, *rest):
    held = rest[-1]
    dates_n, rows_n, cols_n = image.shape
    tiles_n, part_rows = sums.shape[1], sums.shape[2]
    first = part_row(place, k, part_rows)
    end = SUBLANES + part_rows
    tiles = [(t, j, pl.ds(j * LANES, LANES)) for t in range(dates_n) for j in range(tiles_n)]
    for t, j, lanes in tiles:
        held[t, j, SUBLANES:end, :] = image[t, pl.ds(first, part_rows), lanes]

    @pl.when(first > 0)
    def _():
        for t, j, lanes in tiles:
            held[t, j, :SUBLANES, :] = image[t, pl.ds(pl.multiple_of(first - SUBLANES, SUBLANES), SUBLANES), lanes]

    @pl.when(first == 0)
    def _():
        fill_above(place, held, above)

    @pl.when(first + part_rows < rows_n)
    def _():
        for t, j, lanes in tiles:
            held[t, j, end:, :] = image[t, pl.ds(pl.multiple_of(first + part_rows, SUBLANES), SUBLANES), lanes]

    @pl.when(first + part_rows == rows_n)
    def _():
        fill_below(place, held, below)

    @pl.loop(0, part_rows // SUBLANES)
    def _(step):
        row = pl.multiple_of(step * SUBLANES, SUBLANES)
        ratio = [jnp.zeros((SUBLANES, LANES), jnp.float32)] * tiles_n
        for t in range(dates_n):
            total = window_tiles(
                lambda j, d: held[t, j, pl.ds(row + SUBLANES + d, SUBLANES), :], tiles_n
            )
            for j in range(tiles_n):
                sums[t, j, pl.ds(row, SUBLANES), :] = total[j]
                ratio[j] = ratio[j] + held[t, j, pl.ds(row + SUBLANES, SUBLANES), :] / total[j]
        for j in range(tiles_n):
            count = cell_count(place[1] + first + row, j * LANES, rows_total, cols_n)
            part[pl.ds(row, SUBLANES), pl.ds(j * LANES, LANES)] = ratio[j] * count
            if k == 0:
                rest[0][pl.ds(row, SUBLANES), pl.ds(j * LANES, LANES)] = 1.0 / (count * dates_total)


def fill_above(place, held, above):
    keep = (place[2] > 0).astype(jnp.float32)
    for t in range(held.shape[0]):
        for j in range(held.shape[1]):
            held[t, j, SUBLANES - RADIUS : SUBLANES, :] = above[t, :, pl.ds(j * LANES, LANES)] * keep


def fill_below(place, held, below):
    end = held.shape[2] - SUBLANES
    keep = (place[3] > 0).astype(jnp.float32)
    for t in range(held.shape[0]):
        for j in range(held.shape[1]):
            held[t, j, end : end + RADIUS, :] = below[t, :, pl.ds(j * LANES, LANES)] * keep


WHOLE = pl.BlockSpec(memory_space=pltpu.VMEM)
OUTER = pl.BlockSpec(memory_space=pltpu.HBM)


def window_call(image, above, below, k, parts_n, rows_total, dates_total):
    dates_n, rows_n, cols_n = image.shape
    tiles_n = cols_n // LANES
    part_rows = rows_n // parts_n
    outs = 2 if k == 0 else 1
    f32 = jnp.float32
    return pl.pallas_call(
        located(functools.partial(window_kernel, k, rows_total, float(dates_total)), parts_n, rows_n),
        out_shape=[
            jax.ShapeDtypeStruct((dates_n, tiles_n, part_rows, LANES), f32),
        ]
        + [jax.ShapeDtypeStruct((part_rows, cols_n), f32)] * outs,
        in_specs=[WHOLE, WHOLE, WHOLE],
        out_specs=[WHOLE] * (1 + outs),
        scratch_shapes=[pltpu.VMEM((dates_n, tiles_n, part_rows + 2 * SUBLANES, LANES), f32)],
        compiler_params=pltpu.CompilerParams(vmem_limit_bytes=12 * MIB),
        cost_estimate=pl.CostEstimate(flops=500 * image.size, bytes_accessed=8 * image.size, transcendentals=0),
    )(image, above, below)


def change_kernel(parts_n, place, *rest):
    sums = rest[:parts_n]
    change, held, sem = rest[parts_n:]
    dates_n, tiles_n, part_rows, _ = sums[0].shape
    copies = []
    for k in range(parts_n):

        @pl.loop(0, part_rows // SUBLANES)
        def _(step):
            rows = pl.ds(pl.multiple_of(step * SUBLANES, SUBLANES), SUBLANES)
            for j in range(tiles_n):
                before = jnp.log(sums[k][0, j, rows, :])
                for t in range(dates_n - 1):
                    ahead = jnp.log(sums[k][t + 1, j, rows, :])
                    held[k, t, rows, pl.ds(j * LANES, LANES)] = ahead - before
                    before = ahead

        place_rows = pl.ds(part_row(place, k, part_rows), part_rows)
        copy = pltpu.make_async_copy(held.at[k], change.at[pl.ds(0, dates_n - 1), place_rows, :], sem.at[k])
        copy.start()
        copies.append(copy)
    for copy in copies:
        copy.wait()


def change_call(sums):
    parts_n = len(sums)
    dates_n, tiles_n, part_rows, _ = sums[0].shape
    cols_n = tiles_n * LANES
    size = parts_n * sums[0].size
    return pl.pallas_call(
        located(functools.partial(change_kernel, parts_n), parts_n, parts_n * part_rows),
        out_shape=jax.ShapeDtypeStruct((dates_n, parts_n * part_rows, cols_n), jnp.float32),
        in_specs=[WHOLE] * parts_n,
        out_specs=OUTER,
        scratch_shapes=[
            pltpu.VMEM((parts_n, dates_n - 1, part_rows, cols_n), jnp.float32),
            pltpu.SemaphoreType.DMA((parts_n,)),
        ],
        compiler_params=pltpu.CompilerParams(vmem_limit_bytes=12 * MIB),
        cost_estimate=pl.CostEstimate(flops=2000 * size, bytes_accessed=8 * size, transcendentals=size),
        name="change",
    )(*sums)


def last_kernel(parts_n, unroll, place, *rest):
    sums, pieces = rest[:parts_n], rest[parts_n:-7]
    above, below, _, change, held, made, sem = rest[-7:]
    dates_n, tiles_n, part_rows, _ = sums[0].shape
    start = SUBLANES
    for piece in pieces:
        for j in range(tiles_n):
            held[0, j, start : start + piece.shape[1], :] = piece[0, :, pl.ds(j * LANES, LANES)]
        start += piece.shape[1]
    fill_above(place, held, above)
    fill_below(place, held, below)
    keep = place[4] == 0
    for k in range(parts_n):
        first = part_row(place, k, part_rows)

        @pl.loop(0, part_rows // (SUBLANES * unroll))
        def _(step):
            for u in range(unroll):
                inside = pl.multiple_of((step * unroll + u) * SUBLANES, SUBLANES)
                row = pl.multiple_of(first + inside, SUBLANES)
                total = window_tiles(
                    lambda j, d: held[0, j, pl.ds(row + SUBLANES + d, SUBLANES), :], tiles_n
                )
                for j in range(tiles_n):
                    own = sums[k][dates_n - 1, j, pl.ds(inside, SUBLANES), :]
                    ahead = jnp.where(keep, total[j], own)
                    made[pl.ds(row, SUBLANES), pl.ds(j * LANES, LANES)] = jnp.log(ahead) - jnp.log(own)

    copy = pltpu.make_async_copy(made, change.at[dates_n - 1], sem)
    copy.start()
    copy.wait()


def last_call(sums, pieces, above, below, change):
    parts_n = len(sums)
    _, tiles_n, part_rows, _ = sums[0].shape
    rows_n, cols_n = parts_n * part_rows, tiles_n * LANES
    inputs = parts_n + len(pieces) + 2
    unroll = 8 if part_rows % (8 * SUBLANES) == 0 else 1
    return pl.pallas_call(
        located(functools.partial(last_kernel, parts_n, unroll), parts_n, rows_n),
        out_shape=jax.ShapeDtypeStruct(change.shape, jnp.float32),
        in_specs=[WHOLE] * inputs + [OUTER],
        out_specs=OUTER,
        scratch_shapes=[
            pltpu.VMEM((1, tiles_n, rows_n + 2 * SUBLANES, LANES), jnp.float32),
            pltpu.VMEM((rows_n, cols_n), jnp.float32),
            pltpu.SemaphoreType.DMA,
        ],
        input_output_aliases={inputs: 0},
        compiler_params=pltpu.CompilerParams(vmem_limit_bytes=12 * MIB),
        cost_estimate=pl.CostEstimate(flops=2000 * rows_n * cols_n, bytes_accessed=12 * rows_n * cols_n, transcendentals=0),
        name="last",
    )(*sums, *pieces, above, below, change)


def scale_kernel(ks, place, *rest):
    n = len(ks)
    sums, scales = rest[:n], rest[n : 2 * n]
    filtered, held, sem = rest[-3:]
    dates_n, tiles_n, part_rows, _ = sums[0].shape
    copies = []
    for i, k in enumerate(ks):
        rows = pl.ds(part_row(place, k, part_rows), part_rows)
        for t in range(dates_n):
            for j in range(tiles_n):
                lanes = pl.ds(j * LANES, LANES)
                held[i, t, :, lanes] = sums[i][t, j] * scales[i][:, lanes]
            copy = pltpu.make_async_copy(held.at[i, t], filtered.at[t, rows, :], sem.at[i, t])
            copy.start()
            copies.append(copy)
    for copy in copies:
        copy.wait()


def scale_call(sums, scales, ks, rows_n, filtered):
    n = len(ks)
    dates_n, tiles_n, part_rows, _ = sums[0].shape
    cols_n = tiles_n * LANES
    size = n * sums[0].size
    aliased = [] if filtered is None else [filtered]
    return pl.pallas_call(
        located(functools.partial(scale_kernel, ks), rows_n // part_rows, rows_n),
        in_specs=[WHOLE] * (2 * n) + [OUTER] * len(aliased),
        out_specs=OUTER,
        out_shape=jax.ShapeDtypeStruct((dates_n, rows_n, cols_n), jnp.float32),
        scratch_shapes=[
            pltpu.VMEM((n, dates_n, part_rows, cols_n), jnp.float32),
            pltpu.SemaphoreType.DMA((n, dates_n)),
        ],
        input_output_aliases={2 * n: 0} if aliased else {},
        compiler_params=pltpu.CompilerParams(vmem_limit_bytes=12 * MIB),
        cost_estimate=pl.CostEstimate(flops=1000 * size, bytes_accessed=8 * size, transcendentals=0),
    )(*sums, *scales, *aliased)


def crossed(block, axis, bits):
    return lax.ppermute(block, axis, [(i, i ^ bits) for i in range(lax.axis_size(axis))])


def halo_rows(pieces, axis, is_first):
    count = lax.axis_size(axis)
    head = pieces[0][:, :RADIUS]
    tail = pieces[-1][:, pieces[-1].shape[1] - RADIUS :]
    if count == 2:
        other = lax.ppermute(jnp.where(is_first, tail, head), axis, [(0, 1), (1, 0)])
        return other, other
    above = lax.ppermute(tail, axis, [(i, i + 1) for i in range(count - 1)])
    below = lax.ppermute(head, axis, [(i + 1, i) for i in range(count - 1)])
    return above, below


def rim_kernel(place, first, final, rim):
    is_first = place[2] == 0
    rows_n = final.shape[1]
    tail = final[:, rows_n - SUBLANES :, :]
    head = first[:, :SUBLANES, :]
    rim[...] = jnp.where(is_first, tail[:, SUBLANES - RADIUS :, :], head[:, :RADIUS, :])


def rim_call(pieces):
    first, final = pieces[0], pieces[-1]
    return pl.pallas_call(
        located(rim_kernel, 1, final.shape[1]),
        out_shape=jax.ShapeDtypeStruct((first.shape[0], RADIUS, first.shape[2]), jnp.float32),
        in_specs=[WHOLE, WHOLE],
        out_specs=WHOLE,
        compiler_params=pltpu.CompilerParams(vmem_limit_bytes=4 * MIB),
        name="rim",
    )(first, final)


def prepare_kernel(place, image, rim, *rest):
    pieces, (held, sem) = rest[:-2], rest[-2:]
    rows_n = image.shape[1]
    is_first = place[2] == 0
    start = pl.multiple_of(jnp.where(is_first, rows_n - SUBLANES, 0), SUBLANES)
    edge = pltpu.make_async_copy(image.at[:, pl.ds(start, SUBLANES), :], held, sem.at[0])
    edge.start()
    copies, row = [], 0
    for i, piece in enumerate(pieces):
        copy = pltpu.make_async_copy(image.at[pl.ds(0, 1), pl.ds(row, piece.shape[1]), :], piece, sem.at[i + 1])
        copy.start()
        copies.append(copy)
        row += piece.shape[1]
    edge.wait()
    rim[...] = jnp.where(is_first, held[:, SUBLANES - RADIUS :, :], held[:, :RADIUS, :])
    for copy in copies:
        copy.wait()


def prepare_call(image, cuts):
    dates_n, rows_n, cols_n = image.shape
    return pl.pallas_call(
        located(prepare_kernel, 1, rows_n),
        out_shape=[jax.ShapeDtypeStruct((dates_n, RADIUS, cols_n), jnp.float32)]
        + [jax.ShapeDtypeStruct((1, cut, cols_n), jnp.float32) for cut in cuts],
        in_specs=[OUTER],
        out_specs=[WHOLE] * (1 + len(cuts)),
        scratch_shapes=[
            pltpu.VMEM((dates_n, SUBLANES, cols_n), jnp.float32),
            pltpu.SemaphoreType.DMA((1 + len(cuts),)),
        ],
        compiler_params=pltpu.CompilerParams(vmem_limit_bytes=4 * MIB),
        name="prepare",
    )(pltpu.with_memory_space_constraint(image, pltpu.HBM))


def early_rows(rows_n):
    cut = rows_n * 11 // 16 // SUBLANES * SUBLANES
    return cut if cut >= SUBLANES else rows_n


def parts_of(group, rows_n):
    if group & (group - 1):
        return 1
    parts = min(4, group)
    return parts if rows_n % (parts * SUBLANES) == 0 else 1


def on_device(image):
    dates_n, rows_n, _ = image.shape
    row_groups, date_groups = lax.axis_size("row"), lax.axis_size("date")
    row_index = lax.axis_index("row")
    rows_total = rows_n * row_groups
    dates_total = dates_n * date_groups
    parts_n = parts_of(date_groups, rows_n)

    cut = early_rows(rows_n)
    cuts = [cut, rows_n - cut] if cut < rows_n else [cut]
    route = [(i + 1, i) for i in range(date_groups - 1)]
    if row_groups == 2:
        rim, *pieces = prepare_call(image, cuts)
        above = below = lax.ppermute(rim, "row", [(0, 1), (1, 0)])
    else:
        pieces = [image[:1, :cut], image[:1, cut:]][: len(cuts)]
        above, below = halo_rows([image], "row", row_index == 0)
    after = [lax.ppermute(pieces[0], "date", route)]
    if len(pieces) > 1:
        after.append(lax.ppermute(pieces[1], "date", route))
    sums, parts = [], []
    for k in range(parts_n):
        made = window_call(image, above, below, k, parts_n, rows_total, dates_total)
        sums.append(made[0])
        parts.append(made[1])
        if k == 0:
            norm = made[2]

    if parts_n == 1:
        total = lax.psum(parts[0], "date")
    else:
        total = parts[0]
        for k in range(1, parts_n):
            total = total + crossed(parts[k], "date", k)
        bits = parts_n
        while bits < date_groups:
            total = total + crossed(total, "date", bits)
            bits *= 2
    scales = [total * norm]
    for k in range(1, parts_n):
        scales.append(crossed(scales[0], "date", k))

    change = change_call(sums)
    if row_groups == 2:
        after_above = after_below = lax.ppermute(rim_call(after), "row", [(0, 1), (1, 0)])
    else:
        after_above, after_below = halo_rows(after, "row", row_index == 0)
    change = last_call(sums, after, after_above, after_below, change)
    filtered = scale_call(sums[:1], scales[:1], (0,), rows_n, None)
    if parts_n > 1:
        filtered = scale_call(sums[1:], scales[1:], tuple(range(1, parts_n)), rows_n, filtered)
    return filtered, change


def solution(mesh):
    spec = P(("frames", "date"), "row", None)
    return jax.shard_map(on_device, mesh=mesh, in_specs=(spec,), out_specs=(spec, spec), check_vma=False)
```

```python
import functools

import jax
import jax.numpy as jnp
from jax import lax
from jax.experimental import pallas as pl
from jax.experimental.pallas import tpu as pltpu
from jax.sharding import PartitionSpec as P


RADIUS = 3
LANES = 128
SUBLANES = 8
MIB = 1 << 20


def count_1d(places, extent):
    below = jnp.minimum(places, RADIUS)
    above = jnp.minimum(extent - 1 - places, RADIUS)
    return (below + above + 1).astype(jnp.float32)


def cell_count(row, col, rows_total, cols_total):
    shape = (SUBLANES, LANES)
    rows = row + lax.broadcasted_iota(jnp.int32, shape, 0)
    cols = col + lax.broadcasted_iota(jnp.int32, shape, 1)
    return count_1d(rows, rows_total) * count_1d(cols, cols_total)


def lane_shift(tiles, distance):
    lane = lax.broadcasted_iota(jnp.int32, tiles[0].shape, 1)
    zero = jnp.zeros_like(tiles[0])
    turned = [pltpu.roll(tile, (-distance) % LANES, 1) for tile in tiles]
    if distance > 0:
        beside = turned[1:] + [zero]
        own = lane < LANES - distance
    else:
        beside = [zero] + turned[:-1]
        own = lane >= -distance
    return [jnp.where(own, a, b) for a, b in zip(turned, beside)]


def window_tiles(load, tiles_n):
    across = []
    for j in range(tiles_n):
        x = [load(j, k) for k in range(-RADIUS, RADIUS + 1)]
        across.append(((x[0] + x[1]) + (x[2] + x[3])) + ((x[4] + x[5]) + x[6]))
    after = lane_shift(across, 1)
    left = [a + b for a, b in zip(lane_shift(across, -1), across)]
    right = [a + b for a, b in zip(across, after)]
    far_left = lane_shift(left, -2)
    far_right = lane_shift(right, 2)
    return [(far_left[j] + left[j]) + (after[j] + far_right[j]) for j in range(tiles_n)]


def located(kernel, parts_n, rows_n):
    def run(*refs):
        date, row = lax.axis_index("date"), lax.axis_index("row")
        place = [
            date & (parts_n - 1),
            row * rows_n,
            (row > 0).astype(jnp.int32),
            (row < lax.axis_size("row") - 1).astype(jnp.int32),
            (date == lax.axis_size("date") - 1).astype(jnp.int32),
        ]
        return kernel(place, *refs)

    return run


def part_row(place, k, part_rows):
    return pl.multiple_of((place[0] ^ k) * part_rows, SUBLANES)


def window_kernel(ks, rows_total, dates_total, place, image, above, below, *rest):
    held = rest[-1]
    for i, k in enumerate(ks):
        sums, part = rest[2 * i : 2 * i + 2]
        part_windows(k, rows_total, dates_total, place, image, above, below, sums, part, rest[2 * len(ks)], held)


def part_windows(k, rows_total, dates_total, place, image, above, below, sums, part, norm, held):
    dates_n, rows_n, cols_n = image.shape
    tiles_n, part_rows = sums.shape[1], sums.shape[2]
    first = part_row(place, k, part_rows)
    end = SUBLANES + part_rows
    tiles = [(t, j, pl.ds(j * LANES, LANES)) for t in range(dates_n) for j in range(tiles_n)]
    for t, j, lanes in tiles:
        held[t, j, SUBLANES:end, :] = image[t, pl.ds(first, part_rows), lanes]

    @pl.when(first > 0)
    def _():
        for t, j, lanes in tiles:
            held[t, j, :SUBLANES, :] = image[t, pl.ds(pl.multiple_of(first - SUBLANES, SUBLANES), SUBLANES), lanes]

    @pl.when(first == 0)
    def _():
        fill_above(place, held, above)

    @pl.when(first + part_rows < rows_n)
    def _():
        for t, j, lanes in tiles:
            held[t, j, end:, :] = image[t, pl.ds(pl.multiple_of(first + part_rows, SUBLANES), SUBLANES), lanes]

    @pl.when(first + part_rows == rows_n)
    def _():
        fill_below(place, held, below)

    @pl.loop(0, part_rows // SUBLANES)
    def _(step):
        row = pl.multiple_of(step * SUBLANES, SUBLANES)
        ratio = [jnp.zeros((SUBLANES, LANES), jnp.float32)] * tiles_n
        for t in range(dates_n):
            total = window_tiles(
                lambda j, d: held[t, j, pl.ds(row + SUBLANES + d, SUBLANES), :], tiles_n
            )
            for j in range(tiles_n):
                sums[t, j, pl.ds(row, SUBLANES), :] = total[j]
                ratio[j] = ratio[j] + held[t, j, pl.ds(row + SUBLANES, SUBLANES), :] / total[j]
        for j in range(tiles_n):
            count = cell_count(place[1] + first + row, j * LANES, rows_total, cols_n)
            part[pl.ds(row, SUBLANES), pl.ds(j * LANES, LANES)] = ratio[j] * count
            if k == 0:
                norm[pl.ds(row, SUBLANES), pl.ds(j * LANES, LANES)] = 1.0 / (count * dates_total)


def fill_above(place, held, above):
    keep = (place[2] > 0).astype(jnp.float32)
    for t in range(held.shape[0]):
        for j in range(held.shape[1]):
            held[t, j, SUBLANES - RADIUS : SUBLANES, :] = above[t, :, pl.ds(j * LANES, LANES)] * keep


def fill_below(place, held, below):
    end = held.shape[2] - SUBLANES
    keep = (place[3] > 0).astype(jnp.float32)
    for t in range(held.shape[0]):
        for j in range(held.shape[1]):
            held[t, j, end : end + RADIUS, :] = below[t, :, pl.ds(j * LANES, LANES)] * keep


WHOLE = pl.BlockSpec(memory_space=pltpu.VMEM)
OUTER = pl.BlockSpec(memory_space=pltpu.HBM)


def window_call(image, above, below, ks, parts_n, rows_total, dates_total):
    dates_n, rows_n, cols_n = image.shape
    tiles_n = cols_n // LANES
    part_rows = rows_n // parts_n
    f32 = jnp.float32
    sums = jax.ShapeDtypeStruct((dates_n, tiles_n, part_rows, LANES), f32)
    part = jax.ShapeDtypeStruct((part_rows, cols_n), f32)
    out_shape = [sums, part] * len(ks) + [part] * (0 in ks)
    return pl.pallas_call(
        located(functools.partial(window_kernel, ks, rows_total, float(dates_total)), parts_n, rows_n),
        out_shape=out_shape,
        in_specs=[WHOLE, WHOLE, WHOLE],
        out_specs=[WHOLE] * len(out_shape),
        scratch_shapes=[pltpu.VMEM((dates_n, tiles_n, part_rows + 2 * SUBLANES, LANES), f32)],
        compiler_params=pltpu.CompilerParams(vmem_limit_bytes=12 * MIB),
        cost_estimate=pl.CostEstimate(flops=500 * image.size, bytes_accessed=8 * image.size, transcendentals=0),
    )(image, above, below)


def change_kernel(parts_n, place, *rest):
    sums = rest[:parts_n]
    change, held, sem = rest[parts_n:]
    dates_n, tiles_n, part_rows, _ = sums[0].shape
    copies = []
    for k in range(parts_n):

        @pl.loop(0, part_rows // SUBLANES)
        def _(step):
            rows = pl.ds(pl.multiple_of(step * SUBLANES, SUBLANES), SUBLANES)
            for j in range(tiles_n):
                before = jnp.log(sums[k][0, j, rows, :])
                for t in range(dates_n - 1):
                    ahead = jnp.log(sums[k][t + 1, j, rows, :])
                    held[k, t, rows, pl.ds(j * LANES, LANES)] = ahead - before
                    before = ahead

        place_rows = pl.ds(part_row(place, k, part_rows), part_rows)
        copy = pltpu.make_async_copy(held.at[k], change.at[pl.ds(0, dates_n - 1), place_rows, :], sem.at[k])
        copy.start()
        copies.append(copy)
    for copy in copies:
        copy.wait()


def change_call(sums):
    parts_n = len(sums)
    dates_n, tiles_n, part_rows, _ = sums[0].shape
    cols_n = tiles_n * LANES
    size = parts_n * sums[0].size
    return pl.pallas_call(
        located(functools.partial(change_kernel, parts_n), parts_n, parts_n * part_rows),
        out_shape=jax.ShapeDtypeStruct((dates_n, parts_n * part_rows, cols_n), jnp.float32),
        in_specs=[WHOLE] * parts_n,
        out_specs=OUTER,
        scratch_shapes=[
            pltpu.VMEM((parts_n, dates_n - 1, part_rows, cols_n), jnp.float32),
            pltpu.SemaphoreType.DMA((parts_n,)),
        ],
        compiler_params=pltpu.CompilerParams(vmem_limit_bytes=12 * MIB),
        cost_estimate=pl.CostEstimate(flops=2000 * size, bytes_accessed=8 * size, transcendentals=size),
        name="change",
    )(*sums)


def last_kernel(parts_n, unroll, place, *rest):
    sums, pieces = rest[:parts_n], rest[parts_n:-7]
    above, below, _, change, held, made, sem = rest[-7:]
    dates_n, tiles_n, part_rows, _ = sums[0].shape
    start = SUBLANES
    for piece in pieces:
        for j in range(tiles_n):
            held[0, j, start : start + piece.shape[1], :] = piece[0, :, pl.ds(j * LANES, LANES)]
        start += piece.shape[1]
    fill_above(place, held, above)
    fill_below(place, held, below)
    keep = place[4] == 0
    copies = []
    for k in range(parts_n):
        first = part_row(place, k, part_rows)

        @pl.loop(0, part_rows // (SUBLANES * unroll))
        def _(step):
            for u in range(unroll):
                inside = pl.multiple_of((step * unroll + u) * SUBLANES, SUBLANES)
                row = pl.multiple_of(first + inside, SUBLANES)
                total = window_tiles(
                    lambda j, d: held[0, j, pl.ds(row + SUBLANES + d, SUBLANES), :], tiles_n
                )
                for j in range(tiles_n):
                    own = sums[k][dates_n - 1, j, pl.ds(inside, SUBLANES), :]
                    ahead = jnp.where(keep, total[j], own)
                    made[pl.ds(row, SUBLANES), pl.ds(j * LANES, LANES)] = jnp.log(ahead) - jnp.log(own)

        rows = pl.ds(first, part_rows)
        copy = pltpu.make_async_copy(made.at[rows, :], change.at[dates_n - 1, rows, :], sem.at[k])
        copy.start()
        copies.append(copy)
    for copy in copies:
        copy.wait()


def last_call(sums, pieces, above, below, change):
    parts_n = len(sums)
    _, tiles_n, part_rows, _ = sums[0].shape
    rows_n, cols_n = parts_n * part_rows, tiles_n * LANES
    inputs = parts_n + len(pieces) + 2
    unroll = 8 if part_rows % (8 * SUBLANES) == 0 else 1
    return pl.pallas_call(
        located(functools.partial(last_kernel, parts_n, unroll), parts_n, rows_n),
        out_shape=jax.ShapeDtypeStruct(change.shape, jnp.float32),
        in_specs=[WHOLE] * inputs + [OUTER],
        out_specs=OUTER,
        scratch_shapes=[
            pltpu.VMEM((1, tiles_n, rows_n + 2 * SUBLANES, LANES), jnp.float32),
            pltpu.VMEM((rows_n, cols_n), jnp.float32),
            pltpu.SemaphoreType.DMA((parts_n,)),
        ],
        input_output_aliases={inputs: 0},
        compiler_params=pltpu.CompilerParams(vmem_limit_bytes=12 * MIB),
        cost_estimate=pl.CostEstimate(flops=2000 * rows_n * cols_n, bytes_accessed=12 * rows_n * cols_n, transcendentals=0),
        name="last",
    )(*sums, *pieces, above, below, change)


def scale_kernel(ks, place, *rest):
    n = len(ks)
    sums, scales = rest[:n], rest[n : 2 * n]
    filtered, held, sem = rest[-3:]
    dates_n, tiles_n, part_rows, _ = sums[0].shape
    copies = []
    for i, k in enumerate(ks):
        rows = pl.ds(part_row(place, k, part_rows), part_rows)
        for t in range(dates_n):
            for j in range(tiles_n):
                lanes = pl.ds(j * LANES, LANES)
                held[i, t, :, lanes] = sums[i][t, j] * scales[i][:, lanes]
            copy = pltpu.make_async_copy(held.at[i, t], filtered.at[t, rows, :], sem.at[i, t])
            copy.start()
            copies.append(copy)
    for copy in copies:
        copy.wait()


def scale_call(sums, scales, ks, rows_n, filtered):
    n = len(ks)
    dates_n, tiles_n, part_rows, _ = sums[0].shape
    cols_n = tiles_n * LANES
    size = n * sums[0].size
    aliased = [] if filtered is None else [filtered]
    return pl.pallas_call(
        located(functools.partial(scale_kernel, ks), rows_n // part_rows, rows_n),
        in_specs=[WHOLE] * (2 * n) + [OUTER] * len(aliased),
        out_specs=OUTER,
        out_shape=jax.ShapeDtypeStruct((dates_n, rows_n, cols_n), jnp.float32),
        scratch_shapes=[
            pltpu.VMEM((n, dates_n, part_rows, cols_n), jnp.float32),
            pltpu.SemaphoreType.DMA((n, dates_n)),
        ],
        input_output_aliases={2 * n: 0} if aliased else {},
        compiler_params=pltpu.CompilerParams(vmem_limit_bytes=12 * MIB),
        cost_estimate=pl.CostEstimate(flops=1000 * size, bytes_accessed=8 * size, transcendentals=0),
    )(*sums, *scales, *aliased)


def crossed(block, axis, bits):
    return lax.ppermute(block, axis, [(i, i ^ bits) for i in range(lax.axis_size(axis))])


def halo_rows(pieces, axis, is_first):
    count = lax.axis_size(axis)
    head = pieces[0][:, :RADIUS]
    tail = pieces[-1][:, pieces[-1].shape[1] - RADIUS :]
    if count == 2:
        other = lax.ppermute(jnp.where(is_first, tail, head), axis, [(0, 1), (1, 0)])
        return other, other
    above = lax.ppermute(tail, axis, [(i, i + 1) for i in range(count - 1)])
    below = lax.ppermute(head, axis, [(i + 1, i) for i in range(count - 1)])
    return above, below


def rim_kernel(place, first, final, rim):
    is_first = place[2] == 0
    rows_n = final.shape[1]
    tail = final[:, rows_n - SUBLANES :, :]
    head = first[:, :SUBLANES, :]
    rim[...] = jnp.where(is_first, tail[:, SUBLANES - RADIUS :, :], head[:, :RADIUS, :])


def rim_call(pieces):
    first, final = pieces[0], pieces[-1]
    return pl.pallas_call(
        located(rim_kernel, 1, final.shape[1]),
        out_shape=jax.ShapeDtypeStruct((first.shape[0], RADIUS, first.shape[2]), jnp.float32),
        in_specs=[WHOLE, WHOLE],
        out_specs=WHOLE,
        compiler_params=pltpu.CompilerParams(vmem_limit_bytes=4 * MIB),
        name="rim",
    )(first, final)


def prepare_kernel(place, image, rim, *rest):
    pieces, (held, sem) = rest[:-2], rest[-2:]
    rows_n = image.shape[1]
    is_first = place[2] == 0
    start = pl.multiple_of(jnp.where(is_first, rows_n - SUBLANES, 0), SUBLANES)
    edge = pltpu.make_async_copy(image.at[:, pl.ds(start, SUBLANES), :], held, sem.at[0])
    edge.start()
    copies, row = [], 0
    for i, piece in enumerate(pieces):
        copy = pltpu.make_async_copy(image.at[pl.ds(0, 1), pl.ds(row, piece.shape[1]), :], piece, sem.at[i + 1])
        copy.start()
        copies.append(copy)
        row += piece.shape[1]
    edge.wait()
    rim[...] = jnp.where(is_first, held[:, SUBLANES - RADIUS :, :], held[:, :RADIUS, :])
    for copy in copies:
        copy.wait()


def prepare_call(image, cuts):
    dates_n, rows_n, cols_n = image.shape
    return pl.pallas_call(
        located(prepare_kernel, 1, rows_n),
        out_shape=[jax.ShapeDtypeStruct((dates_n, RADIUS, cols_n), jnp.float32)]
        + [jax.ShapeDtypeStruct((1, cut, cols_n), jnp.float32) for cut in cuts],
        in_specs=[OUTER],
        out_specs=[WHOLE] * (1 + len(cuts)),
        scratch_shapes=[
            pltpu.VMEM((dates_n, SUBLANES, cols_n), jnp.float32),
            pltpu.SemaphoreType.DMA((1 + len(cuts),)),
        ],
        compiler_params=pltpu.CompilerParams(vmem_limit_bytes=4 * MIB),
        name="prepare",
    )(pltpu.with_memory_space_constraint(image, pltpu.HBM))


def early_rows(rows_n):
    cut = rows_n * 10 // 16 // SUBLANES * SUBLANES
    return cut if cut >= SUBLANES else rows_n


def parts_of(group, rows_n):
    if group & (group - 1):
        return 1
    parts = min(4, group)
    return parts if rows_n % (parts * SUBLANES) == 0 else 1


def on_device(image):
    dates_n, rows_n, _ = image.shape
    row_groups, date_groups = lax.axis_size("row"), lax.axis_size("date")
    row_index = lax.axis_index("row")
    rows_total = rows_n * row_groups
    dates_total = dates_n * date_groups
    parts_n = parts_of(date_groups, rows_n)

    cut = early_rows(rows_n)
    cuts = [cut, rows_n - cut] if cut < rows_n else [cut]
    route = [(i + 1, i) for i in range(date_groups - 1)]
    if row_groups == 2:
        rim, *pieces = prepare_call(image, cuts)
        above = below = lax.ppermute(rim, "row", [(0, 1), (1, 0)])
    else:
        pieces = [image[:1, :cut], image[:1, cut:]][: len(cuts)]
        above, below = halo_rows([image], "row", row_index == 0)
    after = [lax.ppermute(pieces[0], "date", route)]
    if len(pieces) > 1:
        after.append(lax.ppermute(pieces[1], "date", route))
    others = tuple(range(1, parts_n))
    sums, parts = [None] * parts_n, [None] * parts_n
    for ks in (others, (0,)):
        if ks:
            made = window_call(image, above, below, ks, parts_n, rows_total, dates_total)
            for i, k in enumerate(ks):
                sums[k], parts[k] = made[2 * i : 2 * i + 2]
    norm = made[-1]

    if parts_n == 1:
        total = lax.psum(parts[0], "date")
    else:
        total = parts[0]
        for k in range(1, parts_n):
            total = total + crossed(parts[k], "date", k)
        bits = parts_n
        while bits < date_groups:
            total = total + crossed(total, "date", bits)
            bits *= 2
    scales = [total * norm]
    for k in range(1, parts_n):
        scales.append(crossed(scales[0], "date", k))

    change = change_call(sums)
    if row_groups == 2:
        after_above = after_below = lax.ppermute(rim_call(after), "row", [(0, 1), (1, 0)])
    else:
        after_above, after_below = halo_rows(after, "row", row_index == 0)
    change = last_call(sums, after, after_above, after_below, change)
    filtered = scale_call(sums[:1], scales[:1], (0,), rows_n, None)
    if parts_n > 1:
        filtered = scale_call(sums[1:], scales[1:], tuple(range(1, parts_n)), rows_n, filtered)
    return filtered, change


def solution(mesh):
    spec = P(("frames", "date"), "row", None)
    return jax.shard_map(on_device, mesh=mesh, in_specs=(spec,), out_specs=(spec, spec), check_vma=False)
```
